32 devices in a mesh: src: 4 (over y, x), blk: 8 (over z, core).
Axes of the slice: x: 2, y: 2, z: 4, core: 2. Of those that a mesh axis runs over, the one named last changes fastest.
Arguments:
- values: float32 [4, 512, 32, 128], P('src', 'blk'), may hold values from -0.25 to 0.25
- diagonal: float32 [4, 512, 128], P('src', 'blk'), may hold values from 0.55 to 0.95
- rhs_parts: float32 [4, 512, 128], P('src', 'blk'), may hold values from -24 to 24
- owner_map: int32 [512, 128], P('blk'), may hold values from 0 to 3
- columns: int32 [512, 32, 128], P('blk'), may hold values from 0 to 1073741823
- destination: int32 [512, 1], P('blk'), may hold values from 0 to 7; in each aligned block of 64 rows (0 to 63, 64 to 127, ...) at most 16 rows name the same one
- order_keys: int32 [512], P('blk'), may hold values from 0 to 511, each once
Outputs:
- solution: float32 [512, 128], P('blk')
The draws below stay inside these ranges and needn't reach their ends.
Inputs may be any that keep to these rules, and one draw needn't show every extreme that they name: `destination`: among the row blocks of one index of blk no owner is named more than 16 times, some owner is named exactly 16 times, and every owner is named by some block. `order_keys`: each key appears once.
All inputs are finite; a program needn't handle non-finite values.
Results may differ from the reference program's by a relative error of at most 0.0003.
Values sent between devices are 32-bit elements; how exact they have to be, the bound alone decides.
A program may use at most 64 MiB of HBM per device.

```python
import math
import jax
import jax.numpy as jnp
import numpy as np
from jax import lax

TD = 64
TR = 128
KOFF = 32
SWEEPS = 3
SEND = 16
TILES = 512
N_SRC = 4
N_BLK = 8


def with_ends(array, key, low, top_value):
    index_at = [jax.random.randint(jax.random.fold_in(key, axis), (), 0, length) for axis, length in enumerate(array.shape)]
    widest = array.shape.index(max(array.shape))
    beside = index_at[:widest] + [(index_at[widest] + 1) % array.shape[widest]] + index_at[widest + 1:]
    return array.at[tuple(index_at)].set(low).at[tuple(beside)].set(top_value)


def levels(stream_key, dims, shards, least, high):
    def one(dim, shards_of):
        heights = jax.random.uniform(jax.random.fold_in(jax.random.fold_in(stream_key, 6), dim), (shards_of,), jnp.float32, least / len(shards), high / len(shards))
        return jnp.repeat(jnp.exp(heights), dims[dim] // shards_of).reshape((-1,) + (1,) * (len(dims) - dim - 1))

    gain = one(*shards[0])
    for cut in shards[1:]:
        gain = gain * one(*cut)
    return gain


def routed_block(rng, own, number, rows, number_of, top, most, slope):
    order = jax.random.permutation(rng, number_of)
    crowded, usual = shares(number_of, rows * top, most, slope, True), shares(number_of, rows * top, most, slope, False)
    places = jnp.arange(number_of)

    def named(sizes, rotation):
        used = int((sizes > 0).sum())
        fixed = max(1, used // 4)
        moved = fixed + (places - fixed + rotation * (used - fixed)) % max(1, number_of - fixed)
        return jnp.zeros((number_of,), jnp.int32).at[order[jnp.where(places < fixed, places, moved)]].set(jnp.asarray(sizes, jnp.int32))

    sizes = jnp.where(number % 4 == 0, named(crowded, number // 4), named(usual, number - number // 4 - 1))
    mixed = jax.random.permutation(jax.random.fold_in(own, 3), number_of)
    donor, taker = mixed[0:number_of // 2 * 2:2], mixed[1:number_of // 2 * 2:2]
    room = jnp.minimum(sizes[donor] - 1, most - sizes[taker]) // 2
    room = jnp.where((donor == order[0]) | (taker == order[0]) | (sizes[taker] == 0), 0, jnp.maximum(room, 0))
    moved = jax.random.randint(jax.random.fold_in(own, 4), (number_of // 2,), 0, 1 << 20) % (room + 1)
    sizes = sizes.at[donor].add(-moved).at[taker].add(moved)
    members = jnp.searchsorted(jnp.cumsum(sizes), jnp.arange(rows * top), side="right").astype(jnp.int32)
    listing = members.reshape(top, rows).T
    listing = listing[jax.random.permutation(jax.random.fold_in(own, 1), rows)]
    rotation = jax.random.randint(jax.random.fold_in(own, 2), (rows, 1), 0, top)
    return jnp.take_along_axis(listing, (jnp.arange(top)[None, :] + rotation) % top, axis=1)


def shares(number_of, total, most, slope, full):
    loads = [(1 << 20) // math.isqrt(grade ** slope) + 1 for grade in range(1, number_of + 1)]
    largest = most if full else min(most, max(-(-total // number_of), total * loads[0] // sum(loads)))
    least = 1 if total - largest >= number_of - 1 else 0
    given, spare = [largest] + [least] * (number_of - 1), total - largest - least * (number_of - 1)
    while spare > 0:
        free = [i for i in range(1, number_of) if given[i] < largest] or [i for i in range(1, number_of) if given[i] < most]
        whole, budget = sum([loads[i] for i in free]), spare
        for i in free:
            extra = min(most - given[i], max(1, budget * loads[i] // whole), spare)
            given[i] = given[i] + extra
            spare = spare - extra
    return np.array(given)


def gaussian(rng, dims, scale, limit, shards=(), kind=jnp.bfloat16):
    loudness = levels(rng, dims, shards, -0.22, 0.18) if shards else 1.0
    result = jax.random.normal(rng, dims, jnp.float32) * scale * loudness
    return jnp.minimum(jnp.maximum(result, -limit), limit).astype(kind)


def setup_inputs(seed: int = 0) -> dict:
    splits = jax.random.split(jax.random.key(seed), 8)
    values = jnp.clip(jax.random.uniform(splits[0], (N_SRC, TILES, KOFF, TR), jnp.float32, -0.25, 0.25) * levels(splits[0], (N_SRC, TILES, KOFF, TR), ((0, 4), (1, 8)), -0.4, 0.0), -0.25, 0.25)
    diagonal = jnp.clip(0.55 + 0.39999998 * jax.random.uniform(splits[1], (N_SRC, TILES, TR), jnp.float32) ** levels(splits[1], (N_SRC, TILES, TR), ((0, 4), (1, 8)), -0.2, 0.2), 0.55, 0.95)
    rhs_parts = gaussian(splits[2], (N_SRC, TILES, TR), 4.0, 24.0, ((0, 4), (1, 8)), jnp.float32)
    owner_map = with_ends(jax.random.randint(splits[3], (TILES, TR), 0, N_SRC), jax.random.fold_in(splits[3], 1), 0, N_SRC - 1).astype(jnp.int32)
    columns = with_ends(jax.random.randint(splits[4], (TILES, KOFF, TR), 0, 1073741824), jax.random.fold_in(splits[4], 1), 0, 1073741823).astype(jnp.int32)
    destination_keys = jax.random.split(jax.random.fold_in(splits[5], 1), TILES // TD)
    destination_turns = jax.random.permutation(jax.random.fold_in(splits[5], 3), TILES // TD)
    destination = jax.vmap(lambda own, number: routed_block(jax.random.fold_in(splits[5], 2), own, number, TD, N_BLK, 1, SEND, 2))(destination_keys, destination_turns).reshape((TILES, 1))
    order_keys = jax.random.permutation(splits[6], TILES).astype(jnp.int32)
    return dict(values=values, diagonal=diagonal, rhs_parts=rhs_parts, owner_map=owner_map, columns=columns, destination=destination, order_keys=order_keys)


def reference(values, diagonal, rhs_parts, owner_map, columns, destination, order_keys):
    owner_of = destination[:, 0]
    same_owner = owner_of[:, None] == owner_of[None, :]
    tile_rank = jnp.sum(same_owner & (order_keys[None, :] < order_keys[:, None]), axis=1).astype(jnp.int32)
    owner_ids = jnp.arange(N_BLK, dtype=jnp.int32)
    owner_counts = jnp.sum(owner_of[None, :] == owner_ids[:, None], axis=1).astype(jnp.int32)
    slot_count = N_BLK * SEND
    slot_table = jnp.full((N_BLK, slot_count), -1, jnp.int32)
    slot_table = slot_table.at[owner_of, tile_rank].set(jnp.arange(TILES, dtype=jnp.int32))
    assembled = jnp.sum(values, axis=0)
    assembled_diag = jnp.sum(diagonal, axis=0)
    right_side = jnp.take_along_axis(rhs_parts, owner_map[None, :, :], axis=0)[0]
    slot_numbers = jnp.arange(slot_count, dtype=jnp.int32)

    def solve_owner(owner):
        chosen = slot_table[owner]
        is_live = chosen >= 0
        safe_index = jnp.maximum(chosen, 0)
        block_vals = jnp.where(is_live[:, None, None], assembled[safe_index], 0.0)
        block_cols = columns[safe_index]
        block_right = jnp.where(is_live[:, None], right_side[safe_index], 0.0)
        block_diag = jnp.where(is_live[:, None], assembled_diag[safe_index], 1.0)
        step_over = jnp.remainder(block_cols // TR, 2).astype(jnp.int32)
        target_tile = jnp.remainder(slot_numbers[:, None, None] + step_over, owner_counts[owner]).astype(jnp.int32)
        location = (target_tile * TR + jnp.remainder(block_cols, TR)).astype(jnp.int32)
        iterate = jnp.zeros((slot_count * TR,), jnp.float32)
        for sweep_index in range(SWEEPS):
            nearby = iterate[location]
            summed = jnp.sum(block_vals * nearby, axis=1)
            update = jnp.where(is_live[:, None], (block_right - summed) / block_diag, 0.0)
            iterate = update.reshape(-1)
        return iterate.reshape(slot_count, TR)

    solved = lax.map(solve_owner, owner_ids)
    return solved[owner_of, tile_rank]
```

```python
import functools
import jax
import jax.numpy as jnp
from jax import lax
from jax.experimental import pallas as pl
from jax.experimental.pallas import tpu as pltpu
from jax.sharding import PartitionSpec as P

SWEEPS = 3
FAR = 3.0e38


def kernel(n_src, n_blk, values_hbm, columns_hbm, diag_ref, rhs_ref, map_ref, dest_ref, keys_ref, out_ref,
           vals, cols, comb_all, comb_sum, diag_in, rhs_in, own, zed, picked, nxt, prod, prod_in,
           load_sem, comb_send, comb_recv, dr_send, dr_recv, own_send, own_recv, zed_send, zed_recv,
           nxt_send, nxt_recv, prod_send, prod_recv):
    s = lax.axis_index("src")
    b = lax.axis_index("blk")
    tiles, rows = diag_ref.shape
    stored = vals.shape[1]
    q = tiles // n_src
    lanes = n_blk * q
    total = n_blk * tiles
    src_peers = [lax.rem(s + o, n_src) for o in range(1, n_src)]
    blk_peers = [lax.rem(b + o, n_blk) for o in range(1, n_blk)]
    mesh_id = pl.DeviceIdType.MESH
    started = []

    load_v = pltpu.make_async_copy(values_hbm, vals, load_sem.at[0])
    load_c = pltpu.make_async_copy(columns_hbm, cols, load_sem.at[1])
    load_c.start()
    load_v.start()

    barrier = pltpu.get_barrier_semaphore()
    for peer in src_peers:
        pl.semaphore_signal(barrier, inc=1, device_id={"src": peer}, device_id_type=mesh_id)
    for peer in blk_peers:
        pl.semaphore_signal(barrier, inc=1, device_id={"blk": peer}, device_id_type=mesh_id)

    dest_row = dest_ref[...].astype(jnp.float32)
    comb_row = dest_row * total + keys_ref[...].astype(jnp.float32) + 1.0
    eye = lax.broadcasted_iota(jnp.int32, (tiles, tiles), 0) == lax.broadcasted_iota(jnp.int32, (tiles, tiles), 1)
    comb_col = jnp.sum(jnp.where(eye, comb_row, 0.0), axis=1, keepdims=True)
    low_col = jnp.sum(jnp.where(eye, dest_row, 0.0), axis=1, keepdims=True) * total + 1.0
    at_lane = lax.broadcasted_iota(jnp.int32, (q, lanes), 1) - b * q == lax.broadcasted_iota(jnp.int32, (q, lanes), 0)
    for part in range(n_src):
        spread = jnp.where(at_lane, comb_col[part * q:(part + 1) * q], 0.0)
        comb_all[b, part:part + 1, :] = jnp.sum(spread, axis=0, keepdims=True)

    pl.semaphore_wait(barrier, n_src + n_blk - 2)

    def send(src, dst, send_sem, recv_sem, device):
        copy = pltpu.make_async_remote_copy(src_ref=src, dst_ref=dst, send_sem=send_sem, recv_sem=recv_sem,
                                            device_id=device, device_id_type=mesh_id)
        copy.start()
        started.append(copy)

    def arrive(dst, send_sem, recv_sem, device):
        pltpu.make_async_remote_copy(src_ref=dst, dst_ref=dst, send_sem=send_sem, recv_sem=recv_sem,
                                     device_id=device, device_id_type=mesh_id).wait_recv()

    def rows_of(part):
        return pl.ds(pl.multiple_of(part * q, q), q)

    for peer in src_peers:
        send(diag_ref.at[rows_of(peer)], diag_in.at[s], dr_send.at[0, peer], dr_recv.at[0, s], {"src": peer})
        send(rhs_ref.at[rows_of(peer)], rhs_in.at[s], dr_send.at[1, peer], dr_recv.at[1, s], {"src": peer})
    for peer in blk_peers:
        send(comb_all.at[b], comb_all.at[b], comb_send.at[peer], comb_recv.at[b], {"blk": peer})

    mine = rows_of(s)
    diag_q = diag_ref[mine, :]
    owner_q = map_ref[mine, :]
    right_q = jnp.where(owner_q == s, rhs_ref[mine, :], 0.0)
    for peer in src_peers:
        arrive(diag_in.at[peer], dr_send.at[0, peer], dr_recv.at[0, peer], {"src": peer})
        diag_q = diag_q + diag_in[peer]
        arrive(rhs_in.at[peer], dr_send.at[1, peer], dr_recv.at[1, peer], {"src": peer})
        right_q = jnp.where(owner_q == peer, rhs_in[peer], right_q)

    def share(step, x_q, over_blk):
        own[step, mine, :] = x_q
        if over_blk:
            zed[step, b] = x_q
            for peer in blk_peers:
                send(zed.at[step, b], zed.at[step, b], zed_send.at[step, peer], zed_recv.at[step, b], {"blk": peer})
        for peer in src_peers:
            send(own.at[step, mine], own.at[step, mine], own_send.at[step, peer], own_recv.at[step, s], {"src": peer})

    def own_arrive(step):
        for peer in src_peers:
            arrive(own.at[step, rows_of(peer)], own_send.at[step, peer], own_recv.at[step, peer], {"src": peer})

    def product(step, take, which, first):
        def block(t, carry):
            code = cols[t]
            x = jnp.broadcast_to(take(t), (stored, rows))
            near = jnp.take_along_axis(x, code & (rows - 1), axis=1, mode="promise_in_bounds")
            hit = (code & rows) != 0
            term = jnp.where(hit if which else ~hit, near * vals[t], 0.0)
            row = jnp.sum(term, axis=0, keepdims=True)
            if first:
                prod[step, pl.ds(t, 1), :] = row
            else:
                prod[step, pl.ds(t, 1), :] = prod[step, pl.ds(t, 1), :] + row
            return carry

        lax.fori_loop(0, tiles, block, 0, unroll=8)

    share(0, right_q / diag_q, True)

    for peer in blk_peers:
        arrive(comb_all.at[peer], comb_send.at[peer], comb_recv.at[peer], {"blk": peer})
    all_combs = comb_all[0]
    for other in range(1, n_blk):
        all_combs = all_combs + comb_all[other]
    comb_sum[...] = all_combs
    after = jnp.full((tiles, 1), FAR, jnp.float32)
    least = jnp.full((tiles, 1), FAR, jnp.float32)
    for part in range(n_src):
        line = comb_sum[part:part + 1, :]
        later = (line > comb_col) & (line < low_col + total)
        after = jnp.minimum(after, jnp.min(jnp.where(later, line, FAR), axis=1, keepdims=True))
        least = jnp.minimum(least, jnp.min(jnp.where(line >= low_col, line, FAR), axis=1, keepdims=True))
    follow = jnp.where(after < FAR, after, least)
    choice = jnp.where(comb_sum[pl.ds(s, 1), :] == follow, 1.0, 0.0).astype(jnp.bfloat16)

    load_c.wait()
    load_v.wait()
    for step in range(SWEEPS - 1):
        own_arrive(step)
        product(step, lambda t: own[step, pl.ds(t, 1), :], False, True)
        for peer in blk_peers:
            arrive(zed.at[step, peer], zed_send.at[step, peer], zed_recv.at[step, peer], {"blk": peer})
        spread = zed[step].reshape(lanes, rows)
        high = spread.astype(jnp.bfloat16)
        rest = spread - high.astype(jnp.float32)
        middle = rest.astype(jnp.bfloat16)
        small = (rest - middle.astype(jnp.float32)).astype(jnp.bfloat16)
        got = jnp.dot(choice, high, preferred_element_type=jnp.float32)
        got = got + jnp.dot(choice, middle, preferred_element_type=jnp.float32)
        got = got + jnp.dot(choice, small, preferred_element_type=jnp.float32)
        picked[step] = got
        for peer in src_peers:
            send(picked.at[step], nxt.at[step, s], nxt_send.at[step, peer], nxt_recv.at[step, s], {"src": peer})
        for peer in src_peers:
            arrive(nxt.at[step, peer], nxt_send.at[step, peer], nxt_recv.at[step, peer], {"src": peer})
            got = got + nxt[step, peer]
        nxt[step, s] = got
        product(step, lambda t: nxt[step, s, pl.ds(t, 1), :], True, False)
        for peer in src_peers:
            send(prod.at[step, rows_of(peer)], prod_in.at[step, s], prod_send.at[step, peer], prod_recv.at[step, s], {"src": peer})
        summed = prod[step, mine, :]
        for peer in src_peers:
            arrive(prod_in.at[step, peer], prod_send.at[step, peer], prod_recv.at[step, peer], {"src": peer})
            summed = summed + prod_in[step, peer]
        share(step + 1, (right_q - summed) / diag_q, step < SWEEPS - 2)
    own_arrive(SWEEPS - 1)
    out_ref[...] = own[SWEEPS - 1]
    for copy in started:
        copy.wait_send()


def on_device(values, diagonal, rhs_parts, owner_map, columns, destination, order_keys):
    n_src = lax.axis_size("src")
    n_blk = lax.axis_size("blk")
    tiles, rows = diagonal.shape[1:]
    stored = values.shape[2]
    q = tiles // n_src
    f32 = jnp.float32
    dma = pltpu.SemaphoreType.DMA
    small = pl.BlockSpec(memory_space=pltpu.VMEM)
    big = pl.BlockSpec(memory_space=pl.ANY)
    return pl.pallas_call(
        functools.partial(kernel, n_src, n_blk),
        out_shape=jax.ShapeDtypeStruct((tiles, rows), f32),
        in_specs=[big, big, small, small, small, small, small],
        out_specs=small,
        scratch_shapes=[
            pltpu.VMEM((tiles, stored, rows), f32),
            pltpu.VMEM((tiles, stored, rows), jnp.int32),
            pltpu.VMEM((n_blk, n_src, n_blk * q), f32),
            pltpu.VMEM((n_src, n_blk * q), f32),
            pltpu.VMEM((n_src, q, rows), f32),
            pltpu.VMEM((n_src, q, rows), f32),
            pltpu.VMEM((SWEEPS, tiles, rows), f32),
            pltpu.VMEM((SWEEPS - 1, n_blk, q, rows), f32),
            pltpu.VMEM((SWEEPS - 1, tiles, rows), f32),
            pltpu.VMEM((SWEEPS - 1, n_src, tiles, rows), f32),
            pltpu.VMEM((SWEEPS - 1, tiles, rows), f32),
            pltpu.VMEM((SWEEPS - 1, n_src, q, rows), f32),
            dma((2,)),
            dma((n_blk,)), dma((n_blk,)),
            dma((2, n_src)), dma((2, n_src)),
            dma((SWEEPS, n_src)), dma((SWEEPS, n_src)),
            dma((SWEEPS - 1, n_blk)), dma((SWEEPS - 1, n_blk)),
            dma((SWEEPS - 1, n_src)), dma((SWEEPS - 1, n_src)),
            dma((SWEEPS - 1, n_src)), dma((SWEEPS - 1, n_src)),
        ],
        compiler_params=pltpu.CompilerParams(collective_id=0, has_side_effects=True),
    )(values[0], columns, diagonal[0], rhs_parts[0], owner_map, destination.reshape(1, tiles), order_keys.reshape(1, tiles))


def solution(mesh):
    placed = (
        P("src", "blk", None, None),
        P("src", "blk", None),
        P("src", "blk", None),
        P("blk", None),
        P("blk", None, None),
        P("blk", None),
        P("blk"),
    )
    return jax.shard_map(
        on_device, mesh=mesh, in_specs=placed, out_specs=P("blk", None), check_vma=False
    )
```

```python
import functools
import jax
import jax.numpy as jnp
from jax import lax
from jax.experimental import pallas as pl
from jax.experimental.pallas import tpu as pltpu
from jax.sharding import PartitionSpec as P

SWEEPS = 3
FAR = 3.0e38
CHUNKS = 4
CUTS = (1, 3)


def kernel(n_src, n_blk, values_hbm, columns_hbm, diag_hbm, rhs_hbm, map_hbm, dest_hbm, keys_hbm, out_ref,
           vals, mat_in, cols, diag_ref, rhs_ref, map_ref, dest_ref, keys_ref,
           comb_all, comb_sum, diag_in, rhs_in, zed, picked, nxt, prod, fin,
           load_sem, comb_send, comb_recv, dr_send, dr_recv, out_send, out_recv, zed_send, zed_recv,
           nxt_send, nxt_recv, mat_send, mat_recv):
    s = lax.axis_index("src")
    b = lax.axis_index("blk")
    tiles, rows = diag_ref.shape
    stored = vals.shape[1]
    q = tiles // n_src
    lanes = n_blk * q
    total = n_blk * tiles
    chunk = q // CHUNKS
    src_peers = [lax.rem(s + o, n_src) for o in range(1, n_src)]
    blk_peers = [lax.rem(b + o, n_blk) for o in range(1, n_blk)]
    mesh_id = pl.DeviceIdType.MESH
    started = []

    def rows_of(part):
        return pl.ds(pl.multiple_of(part * q, q), q)

    mine = rows_of(s)
    barrier = pltpu.get_barrier_semaphore()
    for peer in src_peers:
        pl.semaphore_signal(barrier, inc=1, device_id={"src": peer}, device_id_type=mesh_id)
    for peer in blk_peers:
        pl.semaphore_signal(barrier, inc=1, device_id={"blk": peer}, device_id_type=mesh_id)
    pairs = [(dest_hbm, dest_ref), (keys_hbm, keys_ref), (diag_hbm, diag_ref), (rhs_hbm, rhs_ref), (map_hbm, map_ref),
             (columns_hbm.at[mine], cols), (values_hbm.at[mine], vals)]
    loads = [pltpu.make_async_copy(src, dst, load_sem.at[i]) for i, (src, dst) in enumerate(pairs)]
    for load in loads:
        load.start()
    for load in loads[:2]:
        load.wait()

    dest_row = dest_ref[...].astype(jnp.float32)
    comb_row = dest_row * total + keys_ref[...].astype(jnp.float32) + 1.0
    eye = lax.broadcasted_iota(jnp.int32, (tiles, tiles), 0) == lax.broadcasted_iota(jnp.int32, (tiles, tiles), 1)
    comb_col = jnp.sum(jnp.where(eye, comb_row, 0.0), axis=1, keepdims=True)
    low_col = jnp.sum(jnp.where(eye, dest_row, 0.0), axis=1, keepdims=True) * total + 1.0
    at_lane = lax.broadcasted_iota(jnp.int32, (q, lanes), 1) - b * q == lax.broadcasted_iota(jnp.int32, (q, lanes), 0)
    for part in range(n_src):
        spread = jnp.where(at_lane, comb_col[part * q:(part + 1) * q], 0.0)
        comb_all[b, part:part + 1, :] = jnp.sum(spread, axis=0, keepdims=True)
    for load in loads[2:5]:
        load.wait()

    pl.semaphore_wait(barrier, n_src + n_blk - 2)

    def send(src, dst, send_sem, recv_sem, device):
        copy = pltpu.make_async_remote_copy(src_ref=src, dst_ref=dst, send_sem=send_sem, recv_sem=recv_sem,
                                            device_id=device, device_id_type=mesh_id)
        copy.start()
        started.append(copy)

    def arrive(dst, send_sem, recv_sem, device):
        pltpu.make_async_remote_copy(src_ref=dst, dst_ref=dst, send_sem=send_sem, recv_sem=recv_sem,
                                     device_id=device, device_id_type=mesh_id).wait_recv()

    def send_matrix(low, high):
        for piece in range(low, high):
            for peer in src_peers:
                there = pl.ds(pl.multiple_of(peer * q + piece * chunk, chunk), chunk)
                here = pl.ds(piece * chunk, chunk)
                send(values_hbm.at[there], mat_in.at[s, here], mat_send.at[piece, peer], mat_recv.at[piece, s], {"src": peer})

    for peer in src_peers:
        send(diag_ref.at[rows_of(peer)], diag_in.at[s], dr_send.at[0, peer], dr_recv.at[0, s], {"src": peer})
        send(rhs_ref.at[rows_of(peer)], rhs_in.at[s], dr_send.at[1, peer], dr_recv.at[1, s], {"src": peer})
    for peer in blk_peers:
        send(comb_all.at[b], comb_all.at[b], comb_send.at[peer], comb_recv.at[b], {"blk": peer})
    send_matrix(0, CUTS[0])

    diag_q = diag_ref[mine, :]
    owner_q = map_ref[mine, :]
    right_q = jnp.where(owner_q == s, rhs_ref[mine, :], 0.0)
    for peer in src_peers:
        arrive(diag_in.at[peer], dr_send.at[0, peer], dr_recv.at[0, peer], {"src": peer})
        diag_q = diag_q + diag_in[peer]
        arrive(rhs_in.at[peer], dr_send.at[1, peer], dr_recv.at[1, peer], {"src": peer})
        right_q = jnp.where(owner_q == peer, rhs_in[peer], right_q)

    def share(step, x_q):
        zed[step, b] = x_q
        for peer in blk_peers:
            send(zed.at[step, b], zed.at[step, b], zed_send.at[step, peer], zed_recv.at[step, b], {"blk": peer})

    def product(step):
        def block(t, carry):
            code = cols[t]
            if step == 0:
                entry = vals[t]
                for peer in src_peers:
                    entry = entry + mat_in[peer, t]
                vals[t] = entry
            else:
                entry = vals[t]
            lane = code & (rows - 1)
            x = jnp.broadcast_to(zed[step, b, pl.ds(t, 1), :], (stored, rows))
            y = jnp.broadcast_to(nxt[step, s, pl.ds(t, 1), :], (stored, rows))
            near = jnp.take_along_axis(x, lane, axis=1, mode="promise_in_bounds")
            far = jnp.take_along_axis(y, lane, axis=1, mode="promise_in_bounds")
            term = jnp.where((code & rows) != 0, far, near) * entry
            prod[pl.ds(t, 1), :] = jnp.sum(term, axis=0, keepdims=True)
            return carry

        lax.fori_loop(0, q, block, 0, unroll=8)
        return prod[...]

    share(0, right_q / diag_q)
    send_matrix(CUTS[0], CUTS[1])

    for peer in blk_peers:
        arrive(comb_all.at[peer], comb_send.at[peer], comb_recv.at[peer], {"blk": peer})
    all_combs = comb_all[0]
    for other in range(1, n_blk):
        all_combs = all_combs + comb_all[other]
    comb_sum[...] = all_combs
    after = jnp.full((tiles, 1), FAR, jnp.float32)
    least = jnp.full((tiles, 1), FAR, jnp.float32)
    for part in range(n_src):
        line = comb_sum[part:part + 1, :]
        later = (line > comb_col) & (line < low_col + total)
        after = jnp.minimum(after, jnp.min(jnp.where(later, line, FAR), axis=1, keepdims=True))
        least = jnp.minimum(least, jnp.min(jnp.where(line >= low_col, line, FAR), axis=1, keepdims=True))
    follow = jnp.where(after < FAR, after, least)
    choice = jnp.where(comb_sum[pl.ds(s, 1), :] == follow, 1.0, 0.0).astype(jnp.bfloat16)

    for step in range(SWEEPS - 1):
        for peer in blk_peers:
            arrive(zed.at[step, peer], zed_send.at[step, peer], zed_recv.at[step, peer], {"blk": peer})
        spread = zed[step].reshape(lanes, rows)
        high = spread.astype(jnp.bfloat16)
        rest = spread - high.astype(jnp.float32)
        middle = rest.astype(jnp.bfloat16)
        small = (rest - middle.astype(jnp.float32)).astype(jnp.bfloat16)
        got = jnp.dot(choice, high, preferred_element_type=jnp.float32)
        got = got + jnp.dot(choice, middle, preferred_element_type=jnp.float32)
        got = got + jnp.dot(choice, small, preferred_element_type=jnp.float32)
        picked[step] = got
        for peer in src_peers:
            send(picked.at[step, rows_of(peer)], nxt.at[step, s], nxt_send.at[step, peer], nxt_recv.at[step, s], {"src": peer})
        if step == 0:
            send_matrix(CUTS[1], CHUNKS)
            for load in loads[5:]:
                load.wait()
        ahead = picked[step, mine, :]
        for peer in src_peers:
            arrive(nxt.at[step, peer], nxt_send.at[step, peer], nxt_recv.at[step, peer], {"src": peer})
            ahead = ahead + nxt[step, peer]
        nxt[step, s] = ahead
        if step == 0:
            for piece in range(CHUNKS):
                for peer in src_peers:
                    here = pl.ds(piece * chunk, chunk)
                    arrive(mat_in.at[peer, here], mat_send.at[piece, peer], mat_recv.at[piece, peer], {"src": peer})
        x_q = (right_q - product(step)) / diag_q
        if step < SWEEPS - 2:
            share(step + 1, x_q)
    fin[mine, :] = x_q
    for peer in src_peers:
        send(fin.at[mine], fin.at[mine], out_send.at[peer], out_recv.at[s], {"src": peer})
    for peer in src_peers:
        arrive(fin.at[rows_of(peer)], out_send.at[peer], out_recv.at[peer], {"src": peer})
    out_ref[...] = fin[...]
    for copy in started:
        copy.wait_send()


def on_device(values, diagonal, rhs_parts, owner_map, columns, destination, order_keys):
    n_src = lax.axis_size("src")
    n_blk = lax.axis_size("blk")
    tiles, rows = diagonal.shape[1:]
    stored = values.shape[2]
    q = tiles // n_src
    f32 = jnp.float32
    i32 = jnp.int32
    dma = pltpu.SemaphoreType.DMA
    later = SWEEPS - 1
    return pl.pallas_call(
        functools.partial(kernel, n_src, n_blk),
        out_shape=pltpu.VMEM((tiles, rows), f32),
        in_specs=[pl.BlockSpec(memory_space=pl.ANY)] * 7,
        out_specs=pl.BlockSpec(memory_space=pltpu.VMEM),
        scratch_shapes=[
            pltpu.VMEM((q, stored, rows), f32),
            pltpu.VMEM((n_src, q, stored, rows), f32),
            pltpu.VMEM((q, stored, rows), i32),
            pltpu.VMEM((tiles, rows), f32),
            pltpu.VMEM((tiles, rows), f32),
            pltpu.VMEM((tiles, rows), i32),
            pltpu.VMEM((1, tiles), i32),
            pltpu.VMEM((1, tiles), i32),
            pltpu.VMEM((n_blk, n_src, n_blk * q), f32),
            pltpu.VMEM((n_src, n_blk * q), f32),
            pltpu.VMEM((n_src, q, rows), f32),
            pltpu.VMEM((n_src, q, rows), f32),
            pltpu.VMEM((later, n_blk, q, rows), f32),
            pltpu.VMEM((later, tiles, rows), f32),
            pltpu.VMEM((later, n_src, q, rows), f32),
            pltpu.VMEM((q, rows), f32),
            pltpu.VMEM((tiles, rows), f32),
            dma((7,)),
            dma((n_blk,)), dma((n_blk,)),
            dma((2, n_src)), dma((2, n_src)),
            dma((n_src,)), dma((n_src,)),
            dma((later, n_blk)), dma((later, n_blk)),
            dma((later, n_src)), dma((later, n_src)),
            dma((CHUNKS, n_src)), dma((CHUNKS, n_src)),
        ],
        compiler_params=pltpu.CompilerParams(collective_id=0, has_side_effects=True),
    )(values[0], columns, diagonal[0], rhs_parts[0], owner_map, destination.reshape(1, tiles), order_keys.reshape(1, tiles))


def solution(mesh):
    placed = (
        P("src", "blk", None, None),
        P("src", "blk", None),
        P("src", "blk", None),
        P("blk", None),
        P("blk", None, None),
        P("blk", None),
        P("blk"),
    )
    return jax.shard_map(
        on_device, mesh=mesh, in_specs=placed, out_specs=P("blk", None), check_vma=False
    )
```
